512 devices in a mesh: pt: 32 (over y_hi, z), orb: 16 (over x, y_lo, core).
Axes of the slice: x: 4, y: 8 (y_hi: 4, y_lo: 2; y = y_hi * 2 + y_lo), z: 8, core: 2. Of those that a mesh axis runs over, the one named last changes fastest.
Arguments:
- panel_cols: int32 [32], replicated, may hold values from 0 to 16383, as said below
- occ_orbitals: bfloat16 [16384, 2048], P('pt', 'orb'), may hold values from -0.890625 to 0.890625
- vir_orbitals: bfloat16 [16384, 8192], P('pt', 'orb'), may hold values from -0.62890625 to 0.62890625
- occ_energy: float32 [2048], P('orb'), may hold values from 0.05 to 2
- vir_energy: float32 [8192], P('orb'), may hold values from 0.05 to 3
- coulomb: float32 [16384, 16384], P('pt', 'orb'), may hold values from -0.046875 to 0.046875
Outputs:
- screened: float32 [16384, 512], P(('orb', 'pt'))
The draws below stay inside these ranges and needn't reach their ends.
Inputs may be any that keep to these rules, and one draw needn't show every extreme that they name: `panel_cols`: 32 different interpolation point indices.
All inputs are finite; a program needn't handle non-finite values.
Results may differ from the reference program's by a relative error of at most 0.0003.
Values may be sent and summed in bfloat16 or wider, within the bound.
No kernel may reach another device: no remote copies, remote signals or barrier semaphores. Data moves between devices by JAX's collectives and lax.ppermute only.
A program may use at most 64 MiB of HBM per device.

```python
import math
import jax
import jax.numpy as jnp
from jax import lax

NP = 16384
NO = 2048
NV = 8192
NT = 16
NF = 16
NC = 32


def draw_panel_cols(key, part):
    return jax.random.permutation(key, NP)[:NC].astype(jnp.int32)


def block_scale(key, dims, split, least, top_value):
    factor_of, own = 1.0, jax.random.fold_in(key, 6)
    for dim, shards_of in split:
        draws = jnp.exp(jax.random.uniform(jax.random.fold_in(own, dim), (shards_of,), jnp.float32, least / len(split), top_value / len(split)))
        factor_of = factor_of * jnp.repeat(draws, dims[dim] // shards_of).reshape([-1 if axis == dim else 1 for axis in range(len(dims))])
    return factor_of


def gaussian(stream_key, extent, deviation, limit, shards=(), kind=jnp.bfloat16):
    loudness = block_scale(stream_key, extent, shards, -0.22, 0.18) if shards else 1.0
    array = jax.random.normal(stream_key, extent, jnp.float32) * deviation * loudness
    return jnp.minimum(jnp.maximum(array, -limit), limit).astype(kind)


def setup_inputs(seed: int = 0) -> dict:
    arg_keys = jax.random.split(jax.random.key(seed), 7)
    panel_cols = draw_panel_cols(jax.random.fold_in(arg_keys[6], 71), 0)
    occ_orbitals = gaussian(arg_keys[1], (NP, NO), (1.0 / NO ** 0.25), 0.890625, ((0, 32), (1, 16)))
    vir_orbitals = gaussian(arg_keys[2], (NP, NV), (1.0 / NV ** 0.25), 0.62890625, ((0, 32), (1, 16)))
    occ_energy = jnp.clip(jnp.exp(math.log(2.0) - 3.6888794 * jax.random.uniform(arg_keys[3], (NO,), jnp.float32) ** block_scale(arg_keys[3], (NO,), ((0, 16),), -0.2, 0.2)), 0.05, 2.0)
    vir_energy = jnp.clip(jnp.exp(math.log(3.0) - 4.0943445 * jax.random.uniform(arg_keys[4], (NV,), jnp.float32) ** block_scale(arg_keys[4], (NV,), ((0, 16),), -0.2, 0.2)), 0.05, 3.0)
    coulomb = gaussian(arg_keys[5], (NP, NP), NP ** -0.5, 0.046875, ((0, 32), (1, 16)), jnp.float32)
    return dict(panel_cols=panel_cols, occ_orbitals=occ_orbitals, vir_orbitals=vir_orbitals, occ_energy=occ_energy, vir_energy=vir_energy, coulomb=coulomb)


def quadrature():
    moments = 0.05 * jnp.exp(0.3 * jnp.arange(NT, dtype=jnp.float32))
    freqs = 0.1 * jnp.exp(0.3 * jnp.arange(NF, dtype=jnp.float32))
    return moments, 0.3 * moments[None, :] * jnp.cos(freqs[:, None] * moments[None, :])


def scaled_panel(panel_rows, energy, moments):
    decay = jnp.exp(-energy[:, None] * moments[None, :])
    scaled = panel_rows.astype(jnp.float32).T[:, :, None] * decay[:, None, :]
    return scaled.reshape(energy.shape[0], NC * NT).astype(jnp.bfloat16)


def reference(panel_cols, occ_orbitals, vir_orbitals, occ_energy, vir_energy, coulomb):
    moments, cosine_table = quadrature()
    occ_panel = occ_orbitals[panel_cols.astype(jnp.int32)]
    vir_panel = vir_orbitals[panel_cols.astype(jnp.int32)]
    occ_scaled = scaled_panel(occ_panel, occ_energy, moments)
    vir_scaled = scaled_panel(vir_panel, vir_energy, moments)
    green_occ = jnp.dot(occ_orbitals, occ_scaled, preferred_element_type=jnp.float32)
    green_vir = jnp.dot(vir_orbitals, vir_scaled, preferred_element_type=jnp.float32)
    product = (green_occ * green_vir).reshape(NP, NC, NT)
    polar = jnp.einsum('rct,ft->rcf', product, cosine_table, precision=lax.Precision.HIGHEST).reshape(NP, NC * NF)
    return lax.dot_general(coulomb, polar, (((0,), (0,)), ((), ())), precision=lax.Precision.HIGHEST, preferred_element_type=jnp.float32)
```

```python
import jax
import jax.numpy as jnp
import numpy as np
from jax import lax
from jax.sharding import Mesh
from jax.sharding import PartitionSpec as P

NT = 16
NF = 16
NC = 32
RANK = 10
TWICE = 2
WIDTH = 384
SPARE = 127
YZ = ("yh", "z")
ORB = ("x", "yl", "core")
HIGHEST = lax.Precision.HIGHEST
f32, f16, bf16 = jnp.float32, jnp.float16, jnp.bfloat16


def factors():
    moments = 0.05 * np.exp(0.3 * np.arange(NT))
    freqs = 0.1 * np.exp(0.3 * np.arange(NF))
    table = 0.3 * moments[None, :] * np.cos(freqs[:, None] * moments[None, :])
    u = np.linalg.svd(table)[0][:, :RANK]
    rates = np.exp(np.linspace(np.log(0.1), np.log(5.0), 400))
    typical = u.T @ table @ np.exp(-moments[:, None] * rates[None, :])
    turn = np.linalg.eigh(typical @ typical.T)[1][:, ::-1]
    up = u @ turn
    down = up.T @ table
    slots = [*range(TWICE), *range(TWICE), *range(TWICE, RANK)]
    left = np.zeros((NT, NC, len(slots), NC))
    right = np.zeros((len(slots), NC, NC, NF))
    for k, j in enumerate(slots):
        for c in range(NC):
            left[:, c, k, c] = down[j]
            right[k, c, c, :] = up[:, j]
    return (
        left.reshape(NT * NC, WIDTH).astype(np.float32),
        right.reshape(WIDTH, NC * NF).astype(np.float32),
    )


LEFT, RIGHT = factors()


def moved(x, axes):
    return lax.all_to_all(x, axes, split_axis=0, concat_axis=0, tiled=True)


def power_of(x):
    top = jnp.max(jnp.abs(x), axis=-1, keepdims=True)
    return jnp.ceil(jnp.log2(jnp.maximum(top, 1e-30))) - 14.0


def lanes(x):
    return lax.broadcasted_iota(jnp.int32, x.shape, x.ndim - 1)


def packed(x):
    power = power_of(x)
    scaled = x * jnp.exp2(-power)
    lane = lanes(x)
    rest = scaled - lax.reduce_precision(scaled, 5, 10)
    low = (lane >= 64) & (lane < 128)
    return jnp.where(lane == SPARE, power, jnp.where(low, rest, scaled)).astype(f16)


def unpacked(y):
    power = y[..., SPARE : SPARE + 1].astype(f32)
    y = y.astype(f32)
    return jnp.where(lanes(y) == SPARE, 0.0, y) * jnp.exp2(power)


def local(panel_cols, occ_orbitals, vir_orbitals, occ_energy, vir_energy, coulomb):
    moments = 0.05 * jnp.exp(0.3 * jnp.arange(NT, dtype=f32))
    points, no = occ_orbitals.shape
    nv = vir_orbitals.shape[1]
    width = no + nv
    times = NT * NC
    peers = lax.axis_size(ORB)

    base = lax.axis_index(YZ) * points
    positions = lax.broadcasted_iota(jnp.int32, (NC, points), 1)
    selector = (panel_cols[:, None] - base == positions).astype(bf16)
    pick = jnp.concatenate(
        [jnp.dot(selector, o, preferred_element_type=f32).astype(bf16) for o in (occ_orbitals, vir_orbitals)], axis=1
    )
    rows = moved(pick.reshape(NC, width // 128, 128), YZ).astype(f32).sum(axis=0).astype(bf16)
    panel = moved(jnp.broadcast_to(rows, (NC, *rows.shape)), YZ).reshape(NC, width).astype(f32)

    def green(orbitals, energy, panel):
        decay = jnp.exp(-energy[None, :] * moments[:, None])
        scaled = (panel[None] * decay[:, None]).astype(bf16).reshape(times, -1)
        return lax.dot_general(orbitals, scaled, (((1,), (1,)), ((), ())), preferred_element_type=f32)

    occ = green(occ_orbitals, occ_energy, panel[:, :no])
    vir = green(vir_orbitals, vir_energy, panel[:, no:])
    occ_power, vir_power = power_of(occ), power_of(vir)
    lane = lax.broadcasted_iota(jnp.int32, (points, 128), 1)
    sent = jnp.concatenate(
        [
            (occ * jnp.exp2(-occ_power)).astype(f16),
            (vir * jnp.exp2(-vir_power)).astype(f16),
            jnp.where(lane == 0, occ_power, vir_power).astype(f16),
        ],
        axis=1,
    )
    got = moved(sent.reshape(peers, points // peers, -1), ORB)
    occ_power, vir_power = got[..., 2 * times : 2 * times + 1], got[..., 2 * times + 1 : 2 * times + 2]
    occ = (got[..., :times].astype(f32) * jnp.exp2(occ_power.astype(f32))).sum(axis=0)
    vir = (got[..., times : 2 * times].astype(f32) * jnp.exp2(vir_power.astype(f32))).sum(axis=0)
    polar = packed(jnp.dot(occ * vir, LEFT, precision=HIGHEST, preferred_element_type=f32))
    polar = moved(jnp.broadcast_to(polar, (peers, *polar.shape)), ORB)
    polar = unpacked(polar.reshape(points, WIDTH))
    pair = polar[:, :128]
    pair = pair + jnp.roll(pair, 64, axis=1)
    polar = jnp.concatenate([pair, polar[:, 128:]], axis=1)
    part = lax.dot_general(
        coulomb, polar, (((0,), (0,)), ((), ())), precision=lax.Precision.HIGH, preferred_element_type=f32
    )
    blocks = moved(packed(part).reshape(NC, -1, WIDTH), YZ)
    total = unpacked(blocks).sum(axis=0)
    return jnp.dot(total, RIGHT, precision=HIGHEST, preferred_element_type=f32)


def solution(mesh):
    finer = Mesh(mesh.devices.reshape(4, 8, 4, 2, 2), (*YZ, *ORB))
    placed = (P(), P(YZ, ORB), P(YZ, ORB), P(ORB), P(ORB), P(YZ, ORB))
    return jax.shard_map(local, mesh=finer, in_specs=placed, out_specs=P(ORB + YZ, None), check_vma=False)
```

```python
import jax
import jax.numpy as jnp
import numpy as np
from jax import lax
from jax.experimental import pallas as pl
from jax.experimental.layout import Layout, with_layout_constraint
from jax.experimental.pallas import tpu as pltpu
from jax.sharding import Mesh
from jax.sharding import PartitionSpec as P

NT = 16
NF = 16
NC = 32
RANK = 10
TWICE = 2
WIDTH = 384
SPARE = 127
YZ = ("yh", "z")
ORB = ("x", "yl", "core")
HIGHEST = lax.Precision.HIGHEST
f32, f16, bf16 = jnp.float32, jnp.float16, jnp.bfloat16


def factors():
    moments = 0.05 * np.exp(0.3 * np.arange(NT))
    freqs = 0.1 * np.exp(0.3 * np.arange(NF))
    table = 0.3 * moments[None, :] * np.cos(freqs[:, None] * moments[None, :])
    u = np.linalg.svd(table)[0][:, :RANK]
    rates = np.exp(np.linspace(np.log(0.1), np.log(5.0), 400))
    typical = u.T @ table @ np.exp(-moments[:, None] * rates[None, :])
    turn = np.linalg.eigh(typical @ typical.T)[1][:, ::-1]
    up = u @ turn
    down = up.T @ table
    slots = [*range(TWICE), *range(TWICE), *range(TWICE, RANK)]
    left = np.zeros((NT, NC, len(slots), NC))
    right = np.zeros((len(slots), NC, NC, NF))
    for k, j in enumerate(slots):
        for c in range(NC):
            left[:, c, k, c] = down[j]
            right[k, c, c, :] = up[:, j]
    return (
        left.reshape(NT * NC, WIDTH).astype(np.float32),
        right.reshape(WIDTH, NC * NF).astype(np.float32),
    )


LEFT, RIGHT = factors()


def moved(x, axes):
    return lax.all_to_all(x, axes, split_axis=0, concat_axis=0, tiled=True)


def power_of(x):
    top = jnp.max(jnp.abs(x), axis=-1, keepdims=True)
    return jnp.ceil(jnp.log2(jnp.maximum(top, 1e-30))) - 14.0


def lanes(x):
    return lax.broadcasted_iota(jnp.int32, x.shape, x.ndim - 1)


def packed(x):
    power = power_of(x)
    scaled = x * jnp.exp2(-power)
    lane = lanes(x)
    rest = scaled - lax.reduce_precision(scaled, 5, 10)
    low = (lane >= 64) & (lane < 128)
    return jnp.where(lane == SPARE, power, jnp.where(low, rest, scaled)).astype(f16)


def unpacked(y):
    power = y[..., SPARE : SPARE + 1].astype(f32)
    y = y.astype(f32)
    return jnp.where(lanes(y) == SPARE, 0.0, y) * jnp.exp2(power)


def pick_body(cols_ref, occ_ref, vir_ref, out_ref):
    points, no = occ_ref.shape
    base = lax.axis_index(YZ) * points
    column = lax.broadcasted_iota(jnp.int32, (NC, points), 0)
    place = lax.broadcasted_iota(jnp.int32, (NC, points), 1)
    where = jnp.full((NC, points), -1, jnp.int32)
    for c in range(NC):
        where = jnp.where(column == c, cols_ref[c] - base, where)
    chosen = (where == place).astype(f32).astype(bf16)
    occ = jnp.dot(chosen, occ_ref[...], preferred_element_type=f32)
    vir = jnp.dot(chosen, vir_ref[...], preferred_element_type=f32)
    rows = out_ref.shape[1]
    for z in range(out_ref.shape[0]):
        out_ref[z, :, :no] = occ[z * rows : (z + 1) * rows].astype(bf16)
        out_ref[z, :, no:] = vir[z * rows : (z + 1) * rows].astype(bf16)


def plain(x):
    return with_layout_constraint(x, Layout(tuple(range(x.ndim))))


def local(panel_cols, occ_orbitals, vir_orbitals, occ_energy, vir_energy, coulomb):
    moments = 0.05 * jnp.exp(0.3 * jnp.arange(NT, dtype=f32))
    points, no = occ_orbitals.shape
    nv = vir_orbitals.shape[1]
    width = no + nv
    times = NT * NC
    peers = lax.axis_size(ORB)

    zs = lax.axis_size("z")
    pick = pl.pallas_call(
        pick_body,
        out_shape=jax.ShapeDtypeStruct((zs, NC // zs, width), bf16),
        in_specs=[pl.BlockSpec(memory_space=pltpu.SMEM)] + [pl.BlockSpec(memory_space=pltpu.VMEM)] * 2,
    )(panel_cols, occ_orbitals, vir_orbitals)
    own = moved(pick, "z").astype(f32).sum(axis=0).astype(bf16)
    panel = moved(jnp.broadcast_to(own, (lax.axis_size(YZ), *own.shape)), YZ)
    panel = panel.reshape(lax.axis_size("yh"), NC, width).astype(f32).sum(axis=0)

    def green(orbitals, energy, panel):
        decay = jnp.exp(-energy[None, :] * moments[:, None])
        scaled = (panel[None] * decay[:, None]).astype(bf16).reshape(times, -1)
        return plain(lax.dot_general(orbitals, scaled, (((1,), (1,)), ((), ())), preferred_element_type=f32))

    occ = green(occ_orbitals, occ_energy, panel[:, :no])
    vir = green(vir_orbitals, vir_energy, panel[:, no:])
    occ_power, vir_power = power_of(occ), power_of(vir)
    lane = lax.broadcasted_iota(jnp.int32, (points, 128), 1)
    sent = jnp.concatenate(
        [
            (occ * jnp.exp2(-occ_power)).astype(f16),
            (vir * jnp.exp2(-vir_power)).astype(f16),
            jnp.where(lane == 0, occ_power, vir_power).astype(f16),
        ],
        axis=1,
    )
    got = moved(sent.reshape(peers, points // peers, -1), ORB)
    occ_power, vir_power = got[..., 2 * times : 2 * times + 1], got[..., 2 * times + 1 : 2 * times + 2]
    occ = (got[..., :times].astype(f32) * jnp.exp2(occ_power.astype(f32))).sum(axis=0)
    vir = (got[..., times : 2 * times].astype(f32) * jnp.exp2(vir_power.astype(f32))).sum(axis=0)
    polar = packed(jnp.dot(occ * vir, LEFT, precision=HIGHEST, preferred_element_type=f32))
    polar = moved(jnp.broadcast_to(polar, (peers, *polar.shape)), ORB)
    polar = unpacked(polar.reshape(points, WIDTH))
    pair = polar[:, :128]
    pair = pair + jnp.roll(pair, 64, axis=1)
    polar = jnp.concatenate([pair, polar[:, 128:]], axis=1)
    part = lax.dot_general(
        coulomb, polar, (((0,), (0,)), ((), ())), precision=lax.Precision.HIGH, preferred_element_type=f32
    )
    blocks = moved(packed(plain(part)).reshape(NC, -1, WIDTH), YZ)
    total = unpacked(blocks).sum(axis=0)
    return jnp.dot(total, RIGHT, precision=HIGHEST, preferred_element_type=f32)


def solution(mesh):
    finer = Mesh(mesh.devices.reshape(4, 8, 4, 2, 2), (*YZ, *ORB))
    placed = (P(), P(YZ, ORB), P(YZ, ORB), P(ORB), P(ORB), P(YZ, ORB))
    return jax.shard_map(local, mesh=finer, in_specs=placed, out_specs=P(ORB + YZ, None), check_vma=False)
```

```python
import jax
import jax.numpy as jnp
import numpy as np
from jax import lax
from jax.experimental import pallas as pl
from jax.experimental.layout import Layout, with_layout_constraint
from jax.experimental.pallas import tpu as pltpu
from jax.sharding import Mesh
from jax.sharding import PartitionSpec as P

NT = 16
NF = 16
NC = 32
RANK = 10
TWICE = 2
WIDTH = 384
SPARE = 127
SLOTS = 8
YZ = ("yh", "z")
ORB = ("x", "yl", "core")
HIGH = lax.Precision.HIGH
f32, f16, bf16 = jnp.float32, jnp.float16, jnp.bfloat16


def factors():
    moments = 0.05 * np.exp(0.3 * np.arange(NT))
    freqs = 0.1 * np.exp(0.3 * np.arange(NF))
    table = 0.3 * moments[None, :] * np.cos(freqs[:, None] * moments[None, :])
    u = np.linalg.svd(table)[0][:, :RANK]
    rates = np.exp(np.linspace(np.log(0.1), np.log(5.0), 400))
    typical = u.T @ table @ np.exp(-moments[:, None] * rates[None, :])
    turn = np.linalg.eigh(typical @ typical.T)[1][:, ::-1]
    up = u @ turn
    down = up.T @ table
    slots = [*range(TWICE), *range(TWICE), *range(TWICE, RANK)]
    left = np.zeros((NT, NC, len(slots), NC))
    right = np.zeros((len(slots), NC, NC, NF))
    for k, j in enumerate(slots):
        for c in range(NC):
            left[:, c, k, c] = down[j]
            right[k, c, c, :] = up[:, j]
    return (
        left.reshape(NT * NC, WIDTH).astype(np.float32),
        right.reshape(WIDTH, NC * NF).astype(np.float32),
    )


LEFT, RIGHT = factors()


def moved(x, axes):
    return lax.all_to_all(x, axes, split_axis=0, concat_axis=0, tiled=True)


def power_of(x):
    top = jnp.max(jnp.abs(x), axis=-1, keepdims=True)
    return jnp.ceil(jnp.log2(jnp.maximum(top, 1e-30))) - 14.0


def lanes(x):
    return lax.broadcasted_iota(jnp.int32, x.shape, x.ndim - 1)


def at_lane(x, lane):
    return jnp.where(lanes(x) == lane, x, 0).astype(f32).sum(axis=-1, keepdims=True)


def packed(x):
    power = power_of(x)
    scaled = x * jnp.exp2(-power)
    lane = lanes(x)
    rest = scaled - lax.reduce_precision(scaled, 5, 10)
    low = (lane >= 64) & (lane < 128)
    return jnp.where(lane == SPARE, power, jnp.where(low, rest, scaled)).astype(f16)


def unpacked(y):
    power = at_lane(y[..., :128], SPARE)
    y = y.astype(f32)
    return jnp.where(lanes(y) == SPARE, 0.0, y) * jnp.exp2(power)


def pick_body(cols_ref, occ_ref, vir_ref, out_ref):
    points, no = occ_ref.shape
    base = lax.axis_index(YZ) * points
    slot = lax.broadcasted_iota(jnp.int32, (SLOTS, points), 0)
    place = lax.broadcasted_iota(jnp.int32, (SLOTS, points), 1)
    where = jnp.full((SLOTS, points), -1, jnp.int32)
    found = jnp.int32(0)
    for c in range(NC):
        row = cols_ref[c] - base
        here = (row >= 0) & (row < points)
        where = jnp.where(slot == jnp.where(here, found, -1), row, where)
        found = found + here.astype(jnp.int32)
    chosen = (where == place).astype(f32).astype(bf16)
    occ = jnp.dot(chosen, occ_ref[...], preferred_element_type=f32).astype(bf16)
    vir = jnp.dot(chosen, vir_ref[...], preferred_element_type=f32).astype(bf16)
    for k in range(out_ref.shape[0]):
        out_ref[k, :, :no] = occ
        out_ref[k, :, no:] = vir


def plain(x):
    return with_layout_constraint(x, Layout(tuple(range(x.ndim))))


def panel_rows(panel_cols, occ_orbitals, vir_orbitals):
    points, no = occ_orbitals.shape
    width = no + vir_orbitals.shape[1]
    blocks = lax.axis_size(YZ)
    sent = pl.pallas_call(
        pick_body,
        out_shape=jax.ShapeDtypeStruct((blocks, SLOTS, width), bf16),
        in_specs=[pl.BlockSpec(memory_space=pltpu.SMEM)] + [pl.BlockSpec(memory_space=pltpu.VMEM)] * 2,
    )(panel_cols, occ_orbitals, vir_orbitals)
    got = moved(sent, YZ).reshape(blocks * SLOTS, width)
    block = panel_cols // points
    earlier = np.tril(np.ones((NC, NC), bool), -1)
    slot = ((block[:, None] == block[None, :]) & earlier).astype(jnp.int32).sum(axis=1)
    source = lax.broadcasted_iota(jnp.int32, (NC, blocks * SLOTS), 1)
    chosen = ((block * SLOTS + slot)[:, None] == source).astype(bf16)
    few = jnp.dot(chosen, got, preferred_element_type=f32)

    def summed():
        zs = lax.axis_size("z")
        positions = lax.broadcasted_iota(jnp.int32, (NC, points), 1)
        selector = (panel_cols[:, None] - lax.axis_index(YZ) * points == positions).astype(bf16)
        pick = [jnp.dot(selector, o, preferred_element_type=f32).astype(bf16) for o in (occ_orbitals, vir_orbitals)]
        pick = jnp.concatenate(pick, axis=1).reshape(zs, NC // zs, width)
        own = moved(pick, "z").astype(f32).sum(axis=0).astype(bf16)
        rows = moved(jnp.broadcast_to(own, (blocks, *own.shape)), YZ)
        return rows.reshape(-1, NC, width).astype(f32).sum(axis=0)

    return lax.cond(jnp.any(slot >= SLOTS), summed, lambda: few)


def local(panel_cols, occ_orbitals, vir_orbitals, occ_energy, vir_energy, coulomb):
    moments = 0.05 * jnp.exp(0.3 * jnp.arange(NT, dtype=f32))
    points, no = occ_orbitals.shape
    times = NT * NC
    peers = lax.axis_size(ORB)
    panel = panel_rows(panel_cols, occ_orbitals, vir_orbitals)

    def green(orbitals, energy, panel, first):
        decay = jnp.exp(-energy[None, :] * moments[:, None])
        decay = jnp.pad(decay, ((first, 2 * NT + 4 - NT - first), (0, 0)))
        scaled = (panel[None] * decay[:, None]).astype(bf16).reshape(2 * times + 128, -1)
        return lax.dot_general(orbitals, scaled, (((1,), (1,)), ((), ())), preferred_element_type=f32)

    both = green(occ_orbitals, occ_energy, panel[:, :no], 0) + green(vir_orbitals, vir_energy, panel[:, no:], NT)
    both = plain(both)
    power = power_of(both)
    sent = jnp.where(lanes(both) == 2 * times, power, both * jnp.exp2(-power)).astype(f16)
    got = moved(sent.reshape(peers, points // peers, -1), ORB)
    power = at_lane(got[..., 2 * times :], 0)
    both = (got.astype(f32) * jnp.exp2(power)).sum(axis=0)
    product = both[:, :times] * both[:, times : 2 * times]
    polar = packed(jnp.dot(product, LEFT, precision=HIGH, preferred_element_type=f32))
    polar = moved(jnp.broadcast_to(polar, (peers, *polar.shape)), ORB)
    polar = unpacked(polar.reshape(points, WIDTH))
    pair = polar[:, :128]
    pair = pair + jnp.roll(pair, 64, axis=1)
    polar = jnp.concatenate([pair, polar[:, 128:]], axis=1)
    part = lax.dot_general(coulomb, polar, (((0,), (0,)), ((), ())), precision=HIGH, preferred_element_type=f32)
    blocks = moved(packed(plain(part)).reshape(NC, -1, WIDTH), YZ)
    total = unpacked(blocks).sum(axis=0)
    return jnp.dot(total, RIGHT, precision=HIGH, preferred_element_type=f32)


def solution(mesh):
    finer = Mesh(mesh.devices.reshape(4, 8, 4, 2, 2), (*YZ, *ORB))
    placed = (P(), P(YZ, ORB), P(YZ, ORB), P(ORB), P(ORB), P(YZ, ORB))
    return jax.shard_map(local, mesh=finer, in_specs=placed, out_specs=P(ORB + YZ, None), check_vma=False)
```

```python
import jax
import jax.numpy as jnp
import numpy as np
from jax import lax
from jax.experimental import pallas as pl
from jax.experimental.layout import Layout, with_layout_constraint
from jax.experimental.pallas import tpu as pltpu
from jax.sharding import Mesh
from jax.sharding import PartitionSpec as P

NT = 16
NF = 16
NC = 32
RANK = 10
TWICE = 2
WIDTH = 384
SPARE = 127
SLOTS = 8
YZ = ("yh", "z")
ORB = ("x", "yl", "core")
HIGH = lax.Precision.HIGH
f32, f16, bf16 = jnp.float32, jnp.float16, jnp.bfloat16


def factors():
    moments = 0.05 * np.exp(0.3 * np.arange(NT))
    freqs = 0.1 * np.exp(0.3 * np.arange(NF))
    table = 0.3 * moments[None, :] * np.cos(freqs[:, None] * moments[None, :])
    u = np.linalg.svd(table)[0][:, :RANK]
    rates = np.exp(np.linspace(np.log(0.1), np.log(5.0), 400))
    typical = u.T @ table @ np.exp(-moments[:, None] * rates[None, :])
    turn = np.linalg.eigh(typical @ typical.T)[1][:, ::-1]
    up = u @ turn
    down = up.T @ table
    slots = [*range(TWICE), *range(TWICE), *range(TWICE, RANK)]
    left = np.zeros((NT, NC, len(slots), NC))
    right = np.zeros((len(slots), NC, NC, NF))
    for k, j in enumerate(slots):
        for c in range(NC):
            left[:, c, k, c] = down[j]
            right[k, c, c, :] = up[:, j]
    return (
        left.reshape(NT * NC, WIDTH).astype(np.float32),
        right.reshape(WIDTH, NC * NF).astype(np.float32),
    )


LEFT, RIGHT = factors()


def moved(x, axes):
    return lax.all_to_all(x, axes, split_axis=0, concat_axis=0, tiled=True)


def power_of(x):
    top = jnp.max(jnp.abs(x), axis=-1, keepdims=True)
    return jnp.ceil(jnp.log2(jnp.maximum(top, 1e-30))) - 14.0


def lanes(x):
    return lax.broadcasted_iota(jnp.int32, x.shape, x.ndim - 1)


def packed(x):
    power = power_of(x)
    scaled = x * jnp.exp2(-power)
    lane = lanes(x)
    rest = scaled - lax.reduce_precision(scaled, 5, 10)
    low = (lane >= 64) & (lane < 128)
    return jnp.where(lane == SPARE, power, jnp.where(low, rest, scaled)).astype(f16)


def unpacked(y):
    power = y[..., SPARE : SPARE + 1].astype(f32)
    y = y.astype(f32)
    return jnp.where(lanes(y) == SPARE, 0.0, y) * jnp.exp2(power)


def pick_body(cols_ref, occ_ref, vir_ref, out_ref):
    points, no = occ_ref.shape
    base = lax.axis_index(YZ) * points
    slot = lax.broadcasted_iota(jnp.int32, (SLOTS, points), 0)
    place = lax.broadcasted_iota(jnp.int32, (SLOTS, points), 1)
    where = jnp.full((SLOTS, points), -1, jnp.int32)
    found = jnp.int32(0)
    for c in range(NC):
        row = cols_ref[c] - base
        here = (row >= 0) & (row < points)
        where = jnp.where(slot == jnp.where(here, found, -1), row, where)
        found = found + here.astype(jnp.int32)
    chosen = (where == place).astype(f32).astype(bf16)
    occ = jnp.dot(chosen, occ_ref[...], preferred_element_type=f32).astype(bf16)
    vir = jnp.dot(chosen, vir_ref[...], preferred_element_type=f32).astype(bf16)
    for k in range(out_ref.shape[0]):
        out_ref[k, :, :no] = occ
        out_ref[k, :, no:] = vir


def plain(x):
    return with_layout_constraint(x, Layout(tuple(range(x.ndim))))


def panel_rows(panel_cols, occ_orbitals, vir_orbitals):
    points, no = occ_orbitals.shape
    width = no + vir_orbitals.shape[1]
    blocks = lax.axis_size(YZ)
    sent = pl.pallas_call(
        pick_body,
        out_shape=jax.ShapeDtypeStruct((blocks, SLOTS, width), bf16),
        in_specs=[pl.BlockSpec(memory_space=pltpu.SMEM)] + [pl.BlockSpec(memory_space=pltpu.VMEM)] * 2,
    )(panel_cols, occ_orbitals, vir_orbitals)
    got = moved(sent, YZ).reshape(blocks * SLOTS, width)
    block = panel_cols // points
    earlier = np.tril(np.ones((NC, NC), bool), -1)
    slot = ((block[:, None] == block[None, :]) & earlier).astype(jnp.int32).sum(axis=1)
    source = lax.broadcasted_iota(jnp.int32, (NC, blocks * SLOTS), 1)
    chosen = ((block * SLOTS + slot)[:, None] == source).astype(bf16)
    few = jnp.dot(chosen, got, preferred_element_type=f32)

    def summed():
        zs = lax.axis_size("z")
        positions = lax.broadcasted_iota(jnp.int32, (NC, points), 1)
        selector = (panel_cols[:, None] - lax.axis_index(YZ) * points == positions).astype(bf16)
        pick = [jnp.dot(selector, o, preferred_element_type=f32).astype(bf16) for o in (occ_orbitals, vir_orbitals)]
        pick = jnp.concatenate(pick, axis=1).reshape(zs, NC // zs, width)
        own = moved(pick, "z").astype(f32).sum(axis=0).astype(bf16)
        rows = moved(jnp.broadcast_to(own, (blocks, *own.shape)), YZ)
        return rows.reshape(-1, NC, width).astype(f32).sum(axis=0)

    return lax.cond(jnp.any(slot >= SLOTS), summed, lambda: few), sent


def in_three(e):
    hi = lax.reduce_precision(e, 8, 7)
    mid = lax.reduce_precision(e - hi, 8, 7)
    return jnp.stack([hi, mid, e - hi - mid]).astype(bf16)


def to_other_core(x):
    return lax.ppermute(x, "core", [(0, 1), (1, 0)])


def local(panel_cols, occ_orbitals, vir_orbitals, occ_energy, vir_energy, coulomb):
    moments = 0.05 * jnp.exp(0.3 * jnp.arange(NT, dtype=f32))
    points, no = occ_orbitals.shape
    half = points // 2
    times = NT * NC
    core = lax.axis_index("core")

    def rows_of(x, k):
        return jnp.where(k == 0, x[:half], x[half:])

    panel, picked = panel_rows(panel_cols, occ_orbitals, vir_orbitals)
    occ_late, vir_late, _ = lax.optimization_barrier((occ_orbitals, vir_orbitals, picked))
    energies = in_three(jnp.concatenate([occ_energy, vir_energy]))
    theirs = jnp.concatenate([rows_of(occ_late, 1 - core), rows_of(vir_late, 1 - core)], axis=1)
    theirs = jnp.concatenate([theirs, jnp.pad(energies, ((0, 5), (0, 0)))], axis=0)
    theirs = to_other_core(theirs)
    other_panel = to_other_core(panel.astype(bf16)).astype(f32)
    pieces = theirs[half : half + 3].astype(f32)
    other_energy = pieces[0] + pieces[1] + pieces[2]
    theirs = theirs[:half]

    def green(orbitals, energy, panel, first):
        decay = jnp.exp(-energy[None, :] * moments[:, None])
        decay = jnp.pad(decay, ((first, 2 * NT + 4 - NT - first), (0, 0)))
        scaled = (panel[None] * decay[:, None]).astype(bf16).reshape(2 * times + 128, -1)
        return lax.dot_general(orbitals, scaled, (((1,), (1,)), ((), ())), preferred_element_type=f32)

    both = green(rows_of(vir_orbitals, core), vir_energy, panel[:, no:], NT)
    both += green(rows_of(occ_orbitals, core), occ_energy, panel[:, :no], 0)
    both += green(theirs[:, no:], other_energy[no:], other_panel[:, no:], NT)
    both += green(theirs[:, :no], other_energy[:no], other_panel[:, :no], 0)
    both = plain(both)
    power = power_of(both)
    sent = jnp.where(lanes(both) == 2 * times, power, both * jnp.exp2(-power)).astype(f16)
    peers = lax.axis_size(("x", "yl"))
    got = moved(sent.reshape(peers, half // peers, -1), ("x", "yl"))
    power = got[..., 2 * times : 2 * times + 1].astype(f32)
    both = (got.astype(f32) * jnp.exp2(power)).sum(axis=0)
    product = both[:, :times] * both[:, times : 2 * times]
    polar = packed(jnp.dot(product, LEFT, precision=HIGH, preferred_element_type=f32))
    polar = moved(jnp.broadcast_to(polar, (lax.axis_size(ORB), *polar.shape)), ("core", "x", "yl"))
    polar = unpacked(polar.reshape(points, WIDTH))
    pair = polar[:, :128]
    pair = pair + jnp.roll(pair, 64, axis=1)
    polar = jnp.concatenate([pair, polar[:, 128:]], axis=1)
    part = lax.dot_general(coulomb, polar, (((0,), (0,)), ((), ())), precision=HIGH, preferred_element_type=f32)
    blocks = moved(packed(plain(part)).reshape(NC, -1, WIDTH), YZ)
    total = unpacked(blocks).sum(axis=0)
    return jnp.dot(total, RIGHT, precision=HIGH, preferred_element_type=f32)


def solution(mesh):
    finer = Mesh(mesh.devices.reshape(4, 8, 4, 2, 2), (*YZ, *ORB))
    placed = (P(), P(YZ, ORB), P(YZ, ORB), P(ORB), P(ORB), P(YZ, ORB))
    return jax.shard_map(local, mesh=finer, in_specs=placed, out_specs=P(ORB + YZ, None), check_vma=False)
```

```python
import jax
import jax.numpy as jnp
import numpy as np
from jax import lax
from jax.experimental import pallas as pl
from jax.experimental.layout import Layout, with_layout_constraint
from jax.experimental.pallas import tpu as pltpu
from jax.sharding import Mesh
from jax.sharding import PartitionSpec as P

NT = 16
NF = 16
NC = 32
RANK = 10
TWICE = 2
WIDTH = 384
SPARE = 127
SLOTS = 8
YZ = ("yh", "z")
ORB = ("x", "yl", "core")
HIGH = lax.Precision.HIGH
f32, f16, bf16 = jnp.float32, jnp.float16, jnp.bfloat16


def factors():
    moments = 0.05 * np.exp(0.3 * np.arange(NT))
    freqs = 0.1 * np.exp(0.3 * np.arange(NF))
    table = 0.3 * moments[None, :] * np.cos(freqs[:, None] * moments[None, :])
    u = np.linalg.svd(table)[0][:, :RANK]
    rates = np.exp(np.linspace(np.log(0.1), np.log(5.0), 400))
    typical = u.T @ table @ np.exp(-moments[:, None] * rates[None, :])
    turn = np.linalg.eigh(typical @ typical.T)[1][:, ::-1]
    up = u @ turn
    down = up.T @ table
    slots = [*range(TWICE), *range(TWICE), *range(TWICE, RANK)]
    left = np.zeros((NT, NC, len(slots), NC))
    right = np.zeros((len(slots), NC, NC, NF))
    for k, j in enumerate(slots):
        for c in range(NC):
            left[:, c, k, c] = down[j]
            right[k, c, c, :] = up[:, j]
    return (
        left.reshape(NT * NC, WIDTH).astype(np.float32),
        right.reshape(WIDTH, NC * NF).astype(np.float32),
    )


LEFT, RIGHT = factors()
MOMENTS = [float(m) for m in np.float32(0.05) * np.exp(np.float32(0.3) * np.arange(NT, dtype=np.float32))]


def moved(x, axes):
    return lax.all_to_all(x, axes, split_axis=0, concat_axis=0, tiled=True)


def power_of(x):
    top = jnp.max(jnp.abs(x), axis=-1, keepdims=True)
    return jnp.ceil(jnp.log2(jnp.maximum(top, 1e-30))) - 14.0


def lanes(x):
    return lax.broadcasted_iota(jnp.int32, x.shape, x.ndim - 1)


def packed(x):
    power = power_of(x)
    scaled = x * jnp.exp2(-power)
    lane = lanes(x)
    rest = scaled - lax.reduce_precision(scaled, 5, 10)
    low = (lane >= 64) & (lane < 128)
    return jnp.where(lane == SPARE, power, jnp.where(low, rest, scaled)).astype(f16)


def unpacked(y):
    power = y[..., SPARE : SPARE + 1].astype(f32)
    y = y.astype(f32)
    return jnp.where(lanes(y) == SPARE, 0.0, y) * jnp.exp2(power)


def pick_body(cols_ref, occ_ref, vir_ref, out_ref):
    points, no = occ_ref.shape
    base = lax.axis_index(YZ) * points
    slot = lax.broadcasted_iota(jnp.int32, (SLOTS, points), 0)
    place = lax.broadcasted_iota(jnp.int32, (SLOTS, points), 1)
    where = jnp.full((SLOTS, points), -1, jnp.int32)
    found = jnp.int32(0)
    for c in range(NC):
        row = cols_ref[c] - base
        here = (row >= 0) & (row < points)
        where = jnp.where(slot == jnp.where(here, found, -1), row, where)
        found = found + here.astype(jnp.int32)
    chosen = (where == place).astype(f32).astype(bf16)
    occ = jnp.dot(chosen, occ_ref[...], preferred_element_type=f32).astype(bf16)
    vir = jnp.dot(chosen, vir_ref[...], preferred_element_type=f32).astype(bf16)
    for k in range(out_ref.shape[0]):
        out_ref[k, :, :no] = occ
        out_ref[k, :, no:] = vir


def plain(x):
    return with_layout_constraint(x, Layout(tuple(range(x.ndim))))


def on_chip(body, shape, dtype, *args, scratch=()):
    space = pl.BlockSpec(memory_space=pltpu.VMEM)
    return pl.pallas_call(
        body,
        out_shape=pltpu.VMEM(shape, dtype),
        in_specs=[space] * len(args),
        out_specs=space,
        scratch_shapes=scratch,
    )(*[pltpu.with_memory_space_constraint(a, pltpu.VMEM) for a in args])


def green_part(panel, occ_energy, vir_energy, occ, vir, scaled_ref):
    no = occ.shape[1]
    for energy, at in ((occ_energy, slice(0, no)), (vir_energy, slice(no, None))):
        for t in range(NT):
            decay = jnp.exp(-energy * MOMENTS[t])
            scaled_ref[t * NC : (t + 1) * NC, at] = (panel[:, at] * decay).astype(bf16)
    flipped = (((1,), (1,)), ((), ()))
    return (
        lax.dot_general(occ, scaled_ref[:, :no], flipped, preferred_element_type=f32),
        lax.dot_general(vir, scaled_ref[:, no:], flipped, preferred_element_type=f32),
    )


def green_body(panel_ref, other_panel_ref, occ_e_ref, vir_e_ref, other_e_ref, occ_ref, vir_ref, theirs_ref, out_ref, scaled_ref):
    times, no = NT * NC, occ_ref.shape[1]
    half = occ_ref.shape[0]
    occ, vir = green_part(panel_ref[...], occ_e_ref[...], vir_e_ref[...], occ_ref[...], vir_ref[...], scaled_ref.at[0])
    energy, theirs = other_e_ref[...], theirs_ref[:half]
    other_occ, other_vir = green_part(
        other_panel_ref[...].astype(f32),
        energy[:, :no],
        energy[:, no:],
        theirs[:, :no],
        theirs[:, no:],
        scaled_ref.at[1],
    )
    occ, vir = occ + other_occ, vir + other_vir
    power = jnp.maximum(power_of(occ), power_of(vir))
    factor = jnp.exp2(-power)
    out_ref[:, :times] = occ * factor
    out_ref[:, times : 2 * times] = vir * factor
    out_ref[:, 2 * times :] = jnp.broadcast_to(power, (occ.shape[0], 128))


def panel_rows(panel_cols, occ_orbitals, vir_orbitals):
    points, no = occ_orbitals.shape
    width = no + vir_orbitals.shape[1]
    blocks = lax.axis_size(YZ)
    sent = pl.pallas_call(
        pick_body,
        out_shape=jax.ShapeDtypeStruct((blocks, SLOTS, width), bf16),
        in_specs=[pl.BlockSpec(memory_space=pltpu.SMEM)] + [pl.BlockSpec(memory_space=pltpu.VMEM)] * 2,
    )(panel_cols, occ_orbitals, vir_orbitals)
    got = moved(sent, YZ).reshape(blocks * SLOTS, width)
    block = panel_cols // points
    earlier = np.tril(np.ones((NC, NC), bool), -1)
    slot = ((block[:, None] == block[None, :]) & earlier).astype(jnp.int32).sum(axis=1)
    source = lax.broadcasted_iota(jnp.int32, (NC, blocks * SLOTS), 1)
    chosen = ((block * SLOTS + slot)[:, None] == source).astype(bf16)
    few = jnp.dot(chosen, got, preferred_element_type=f32)

    def summed():
        zs = lax.axis_size("z")
        positions = lax.broadcasted_iota(jnp.int32, (NC, points), 1)
        selector = (panel_cols[:, None] - lax.axis_index(YZ) * points == positions).astype(bf16)
        pick = [jnp.dot(selector, o, preferred_element_type=f32).astype(bf16) for o in (occ_orbitals, vir_orbitals)]
        pick = jnp.concatenate(pick, axis=1).reshape(zs, NC // zs, width)
        own = moved(pick, "z").astype(f32).sum(axis=0).astype(bf16)
        rows = moved(jnp.broadcast_to(own, (blocks, *own.shape)), YZ)
        return rows.reshape(-1, NC, width).astype(f32).sum(axis=0)

    return lax.cond(jnp.any(slot >= SLOTS), summed, lambda: few), sent


def in_three(e):
    hi = lax.reduce_precision(e, 8, 7)
    mid = lax.reduce_precision(e - hi, 8, 7)
    return jnp.stack([hi, mid, e - hi - mid]).astype(bf16)


def to_other_core(x):
    return lax.ppermute(x, "core", [(0, 1), (1, 0)])


def local(panel_cols, occ_orbitals, vir_orbitals, occ_energy, vir_energy, coulomb):
    points, no = occ_orbitals.shape
    half = points // 2
    times = NT * NC
    core = lax.axis_index("core")

    def rows_of(x, k):
        return jnp.where(k == 0, x[:half], x[half:])

    panel, picked = panel_rows(panel_cols, occ_orbitals, vir_orbitals)
    occ_late, vir_late, _ = lax.optimization_barrier((occ_orbitals, vir_orbitals, picked))
    right = lax.optimization_barrier(RIGHT + 0.0 * picked[0, 0, 0].astype(f32))
    energies = in_three(jnp.concatenate([occ_energy, vir_energy]))
    theirs = jnp.concatenate([rows_of(occ_late, 1 - core), rows_of(vir_late, 1 - core)], axis=1)
    theirs = jnp.concatenate([theirs, jnp.pad(energies, ((0, 5), (0, 0)))], axis=0)
    theirs = to_other_core(theirs)
    pieces = theirs[half : half + 3].astype(f32)
    other_energy = pieces[0:1] + pieces[1:2] + pieces[2:3]
    other_panel = to_other_core(panel.astype(bf16))
    sent = on_chip(
        green_body,
        (half, 2 * times + 128),
        f32,
        panel,
        other_panel,
        occ_energy.reshape(1, -1),
        vir_energy.reshape(1, -1),
        other_energy,
        rows_of(occ_late, core),
        rows_of(vir_late, core),
        theirs,
        scratch=[pltpu.VMEM((2, times, panel.shape[1]), bf16)],
    ).astype(f16)
    peers = lax.axis_size(("x", "yl"))
    got = moved(sent.reshape(peers, half // peers, -1), ("x", "yl"))
    power = got[..., 2 * times : 2 * times + 1].astype(f32)
    both = (got.astype(f32) * jnp.exp2(power)).sum(axis=0)
    product, right = lax.optimization_barrier((both[:, :times] * both[:, times : 2 * times], right))
    polar = packed(jnp.dot(product, LEFT, precision=HIGH, preferred_element_type=f32))
    polar = moved(jnp.broadcast_to(polar, (lax.axis_size(ORB), *polar.shape)), ("core", "x", "yl"))
    polar = unpacked(polar.reshape(points, WIDTH))
    pair = polar[:, :128]
    pair = pair + jnp.roll(pair, 64, axis=1)
    polar = jnp.concatenate([pair, polar[:, 128:]], axis=1)
    part = lax.dot_general(coulomb, polar, (((0,), (0,)), ((), ())), precision=HIGH, preferred_element_type=f32)
    blocks = moved(packed(plain(part)).reshape(NC, -1, WIDTH), YZ)
    total = unpacked(blocks).sum(axis=0)
    return jnp.dot(total, right, precision=HIGH, preferred_element_type=f32)


def solution(mesh):
    finer = Mesh(mesh.devices.reshape(4, 8, 4, 2, 2), (*YZ, *ORB))
    placed = (P(), P(YZ, ORB), P(YZ, ORB), P(ORB), P(ORB), P(YZ, ORB))
    return jax.shard_map(local, mesh=finer, in_specs=placed, out_specs=P(ORB + YZ, None), check_vma=False)
```

```python
import jax
import jax.numpy as jnp
import numpy as np
from jax import lax
from jax.experimental import pallas as pl
from jax.experimental.pallas import tpu as pltpu
from jax.sharding import Mesh
from jax.sharding import PartitionSpec as P

NT = 16
NF = 16
NC = 32
RANK = 10
TWICE = 2
WIDTH = 384
SPARE = 127
SLOTS = 8
VMEM_LIMIT = 12 * 2**20
YZ = ("yh", "z")
ORB = ("x", "yl", "core")
f32, f16, bf16 = jnp.float32, jnp.float16, jnp.bfloat16


def factors():
    moments = 0.05 * np.exp(0.3 * np.arange(NT))
    freqs = 0.1 * np.exp(0.3 * np.arange(NF))
    table = 0.3 * moments[None, :] * np.cos(freqs[:, None] * moments[None, :])
    u = np.linalg.svd(table)[0][:, :RANK]
    rates = np.exp(np.linspace(np.log(0.1), np.log(5.0), 400))
    typical = u.T @ table @ np.exp(-moments[:, None] * rates[None, :])
    turn = np.linalg.eigh(typical @ typical.T)[1][:, ::-1]
    up = u @ turn
    down = up.T @ table
    slots = [*range(TWICE), *range(TWICE), *range(TWICE, RANK)]
    return np.repeat(down[slots].T, NC, axis=1).astype(np.float32), np.tile(up[:, slots].T, (1, NC)).astype(np.float32)


DOWN, UP = factors()
MOMENTS = [float(m) for m in np.float32(0.05) * np.exp(np.float32(0.3) * np.arange(NT, dtype=np.float32))]


def moved(x, axes):
    return lax.all_to_all(x, axes, split_axis=0, concat_axis=0, tiled=True)


def power_of(x):
    top = jnp.max(jnp.abs(x), axis=-1, keepdims=True)
    return jnp.ceil(jnp.log2(jnp.maximum(top, 1e-30))) - 14.0


def lanes(x):
    return lax.broadcasted_iota(jnp.int32, x.shape, x.ndim - 1)


def spread(x):
    power = power_of(x)
    scaled = x * jnp.exp2(-power)
    wide = scaled * 8193.0
    high = wide - (wide - scaled)
    lane = lanes(x)
    scaled = jnp.where(lane < 64, high, jnp.where(lane < 128, scaled - high, scaled))
    return jnp.where(lane == SPARE, power, scaled)


def unpacked(y):
    power = y[:, SPARE : SPARE + 1]
    return jnp.where(lanes(y) == SPARE, 0.0, y) * jnp.exp2(power)


def two_parts(x):
    high = x.astype(bf16)
    return high, (x - high.astype(f32)).astype(bf16)


def product_of(x, y):
    (a, b), (c, d) = x, y
    total = jnp.dot(a, c, preferred_element_type=f32)
    total += jnp.dot(a, d, preferred_element_type=f32)
    return total + jnp.dot(b, c, preferred_element_type=f32)


def pick_body(cols_ref, occ_ref, vir_ref, out_ref):
    points, no = occ_ref.shape
    base = lax.axis_index(YZ) * points
    slot = lax.broadcasted_iota(jnp.int32, (SLOTS, points), 0)
    place = lax.broadcasted_iota(jnp.int32, (SLOTS, points), 1)
    where = jnp.full((SLOTS, points), -1, jnp.int32)
    found = jnp.int32(0)
    for c in range(NC):
        row = cols_ref[c] - base
        here = (row >= 0) & (row < points)
        where = jnp.where(slot == jnp.where(here, found, -1), row, where)
        found = found + here.astype(jnp.int32)
    chosen = (where == place).astype(f32).astype(bf16)
    occ = jnp.dot(chosen, occ_ref[...], preferred_element_type=f32).astype(bf16)
    vir = jnp.dot(chosen, vir_ref[...], preferred_element_type=f32).astype(bf16)
    for k in range(out_ref.shape[0]):
        out_ref[k, :, :no] = occ
        out_ref[k, :, no:] = vir


def on_chip(body, shape, dtype, *args, scratch=(), last=False):
    space = pl.BlockSpec(memory_space=pltpu.VMEM)
    return pl.pallas_call(
        body,
        out_shape=jax.ShapeDtypeStruct(shape, dtype) if last else pltpu.VMEM(shape, dtype),
        in_specs=[space] * len(args),
        out_specs=space,
        scratch_shapes=scratch,
        compiler_params=pltpu.CompilerParams(vmem_limit_bytes=VMEM_LIMIT),
    )(*[pltpu.with_memory_space_constraint(jnp.asarray(a), pltpu.VMEM) for a in args])


def green_part(panel, occ_energy, vir_energy, occ, vir, scaled_ref):
    no = occ.shape[1]
    for energy, at in ((occ_energy, slice(0, no)), (vir_energy, slice(no, None))):
        for t in range(NT):
            decay = jnp.exp(-energy * MOMENTS[t])
            scaled_ref[t * NC : (t + 1) * NC, at] = (panel[:, at] * decay).astype(bf16)
    flipped = (((1,), (1,)), ((), ()))
    return (
        lax.dot_general(occ, scaled_ref[:, :no], flipped, preferred_element_type=f32),
        lax.dot_general(vir, scaled_ref[:, no:], flipped, preferred_element_type=f32),
    )


def green_body(panel_ref, other_panel_ref, occ_e_ref, vir_e_ref, other_e_ref, occ_ref, vir_ref, theirs_ref, out_ref, scaled_ref):
    times, no = NT * NC, occ_ref.shape[1]
    half = occ_ref.shape[0]
    occ, vir = green_part(panel_ref[...], occ_e_ref[...], vir_e_ref[...], occ_ref[...], vir_ref[...], scaled_ref.at[0])
    energy, theirs = other_e_ref[...], theirs_ref[:half]
    other_occ, other_vir = green_part(
        other_panel_ref[...].astype(f32),
        energy[:, :no],
        energy[:, no:],
        theirs[:, :no],
        theirs[:, no:],
        scaled_ref.at[1],
    )
    occ, vir = occ + other_occ, vir + other_vir
    power = jnp.maximum(power_of(occ), power_of(vir))
    factor = jnp.exp2(-power)
    out_ref[:, :times] = occ * factor
    out_ref[:, times : 2 * times] = vir * factor
    out_ref[:, 2 * times :] = jnp.broadcast_to(power, (occ.shape[0], 128))


def polar_body(got_ref, down_ref, out_ref, table_ref):
    times = NT * NC
    occ, vir = 0.0, 0.0
    for k in range(got_ref.shape[0]):
        factor = jnp.exp2(got_ref[k, :, 2 * times : 2 * times + 1])
        occ += got_ref[k, :, :times] * factor
        vir += got_ref[k, :, times : 2 * times] * factor
    column = lax.broadcasted_iota(jnp.int32, (NC, WIDTH), 0)
    same = (column == lax.broadcasted_iota(jnp.int32, (NC, WIDTH), 1) % NC).astype(f32)
    for t in range(NT):
        table_ref[t * NC : (t + 1) * NC, :] = same * down_ref[t : t + 1, :]
    out_ref[...] = spread(product_of(two_parts(occ * vir), two_parts(table_ref[...])))


def screen_body(coulomb_ref, polar_ref, out_ref):
    polar = unpacked(polar_ref[...])
    pair = polar[:, :128]
    polar = two_parts(jnp.concatenate([pair + pltpu.roll(pair, 64, 1), polar[:, 128:]], axis=1))
    step = 256
    for at in range(0, out_ref.shape[0], step):
        block = two_parts(coulomb_ref[:, at : at + step].T)
        out_ref[at : at + step, :] = spread(product_of(block, polar))


def total_body(blocks_ref, up_ref, out_ref, table_ref):
    total = 0.0
    for k in range(blocks_ref.shape[0]):
        total += unpacked(blocks_ref[k])
    column = lax.broadcasted_iota(jnp.int32, (NC, NC * NF), 0)
    same = (column == lax.broadcasted_iota(jnp.int32, (NC, NC * NF), 1) // NF).astype(f32)
    for k in range(WIDTH // NC):
        table_ref[k * NC : (k + 1) * NC, :] = same * up_ref[k : k + 1, :]
    out_ref[...] = product_of(two_parts(total), two_parts(table_ref[...]))


def panel_rows(panel_cols, occ_orbitals, vir_orbitals):
    points, no = occ_orbitals.shape
    width = no + vir_orbitals.shape[1]
    blocks = lax.axis_size(YZ)
    sent = pl.pallas_call(
        pick_body,
        out_shape=jax.ShapeDtypeStruct((blocks, SLOTS, width), bf16),
        in_specs=[pl.BlockSpec(memory_space=pltpu.SMEM)] + [pl.BlockSpec(memory_space=pltpu.VMEM)] * 2,
        compiler_params=pltpu.CompilerParams(vmem_limit_bytes=VMEM_LIMIT),
    )(panel_cols, occ_orbitals, vir_orbitals)
    got = moved(sent, YZ).reshape(blocks * SLOTS, width)
    block = panel_cols // points
    earlier = np.tril(np.ones((NC, NC), bool), -1)
    slot = ((block[:, None] == block[None, :]) & earlier).astype(jnp.int32).sum(axis=1)
    source = lax.broadcasted_iota(jnp.int32, (NC, blocks * SLOTS), 1)
    chosen = ((block * SLOTS + slot)[:, None] == source).astype(bf16)
    few = jnp.dot(chosen, got, preferred_element_type=f32)

    def summed():
        zs = lax.axis_size("z")
        positions = lax.broadcasted_iota(jnp.int32, (NC, points), 1)
        selector = (panel_cols[:, None] - lax.axis_index(YZ) * points == positions).astype(bf16)
        pick = [jnp.dot(selector, o, preferred_element_type=f32).astype(bf16) for o in (occ_orbitals, vir_orbitals)]
        pick = jnp.concatenate(pick, axis=1).reshape(zs, NC // zs, width)
        own = moved(pick, "z").astype(f32).sum(axis=0).astype(bf16)
        rows = moved(jnp.broadcast_to(own, (blocks, *own.shape)), YZ)
        return rows.reshape(-1, NC, width).astype(f32).sum(axis=0)

    return lax.cond(jnp.any(slot >= SLOTS), summed, lambda: few), sent


def in_three(e):
    hi = lax.reduce_precision(e, 8, 7)
    mid = lax.reduce_precision(e - hi, 8, 7)
    return jnp.stack([hi, mid, e - hi - mid]).astype(bf16)


def to_other_core(x):
    return lax.ppermute(x, "core", [(0, 1), (1, 0)])


def local(panel_cols, occ_orbitals, vir_orbitals, occ_energy, vir_energy, coulomb):
    points, no = occ_orbitals.shape
    half = points // 2
    times = NT * NC
    core = lax.axis_index("core")

    def rows_of(x, k):
        return jnp.where(k == 0, x[:half], x[half:])

    panel, picked = panel_rows(panel_cols, occ_orbitals, vir_orbitals)
    occ_late, vir_late, _ = lax.optimization_barrier((occ_orbitals, vir_orbitals, picked))
    coulomb = coulomb + 0.0 * picked[0, 0, 0].astype(f32)
    panel, coulomb = lax.optimization_barrier((panel, coulomb))
    energies = in_three(jnp.concatenate([occ_energy, vir_energy]))
    theirs = jnp.concatenate([rows_of(occ_late, 1 - core), rows_of(vir_late, 1 - core)], axis=1)
    theirs = jnp.concatenate([theirs, jnp.pad(energies, ((0, 5), (0, 0)))], axis=0)
    theirs = to_other_core(theirs)
    pieces = theirs[half : half + 3].astype(f32)
    other_energy = pieces[0:1] + pieces[1:2] + pieces[2:3]
    other_panel = to_other_core(panel.astype(bf16))
    sent = on_chip(
        green_body,
        (half, 2 * times + 128),
        f32,
        panel,
        other_panel,
        occ_energy.reshape(1, -1),
        vir_energy.reshape(1, -1),
        other_energy,
        rows_of(occ_late, core),
        rows_of(vir_late, core),
        theirs,
        scratch=[pltpu.VMEM((2, times, panel.shape[1]), bf16)],
    ).astype(f16)
    peers = lax.axis_size(("x", "yl"))
    got = moved(sent.reshape(peers, half // peers, -1), ("x", "yl"))
    table = [pltpu.VMEM((times, WIDTH), f32)]
    polar = on_chip(polar_body, (got.shape[1], WIDTH), f32, got.astype(f32), DOWN, scratch=table).astype(f16)
    polar = moved(jnp.broadcast_to(polar, (lax.axis_size(ORB), *polar.shape)), ("core", "x", "yl"))
    polar = polar.reshape(points, WIDTH).astype(f32)
    part = on_chip(screen_body, (coulomb.shape[1], WIDTH), f32, coulomb, polar).astype(f16)
    blocks = moved(part.reshape(NC, -1, WIDTH), YZ).astype(f32)
    table = [pltpu.VMEM((WIDTH, NC * NF), f32)]
    return on_chip(total_body, (blocks.shape[1], NC * NF), f32, blocks, UP, scratch=table, last=True)


def solution(mesh):
    finer = Mesh(mesh.devices.reshape(4, 8, 4, 2, 2), (*YZ, *ORB))
    placed = (P(), P(YZ, ORB), P(YZ, ORB), P(ORB), P(ORB), P(YZ, ORB))
    return jax.shard_map(local, mesh=finer, in_specs=placed, out_specs=P(ORB + YZ, None), check_vma=False)
```

```python
import functools

import jax
import jax.numpy as jnp
import numpy as np
from jax import lax
from jax.experimental import pallas as pl
from jax.experimental.pallas import tpu as pltpu
from jax.sharding import Mesh
from jax.sharding import PartitionSpec as P

NT = 16
NF = 16
NC = 32
RANK = 10
TWICE = 2
WIDTH = 384
SPARE = 127
SLOTS = 8
VMEM_LIMIT = 12 * 2**20
YZ = ("yh", "z")
ORB = ("x", "yl", "core")
QUARTET = ("yl", "core")
f32, f16, bf16 = jnp.float32, jnp.float16, jnp.bfloat16


def factors():
    moments = 0.05 * np.exp(0.3 * np.arange(NT))
    freqs = 0.1 * np.exp(0.3 * np.arange(NF))
    table = 0.3 * moments[None, :] * np.cos(freqs[:, None] * moments[None, :])
    u = np.linalg.svd(table)[0][:, :RANK]
    rates = np.exp(np.linspace(np.log(0.1), np.log(5.0), 400))
    typical = u.T @ table @ np.exp(-moments[:, None] * rates[None, :])
    turn = np.linalg.eigh(typical @ typical.T)[1][:, ::-1]
    up = u @ turn
    down = up.T @ table
    slots = [*range(TWICE), *range(TWICE), *range(TWICE, RANK)]
    return np.repeat(down[slots].T, NC, axis=1).astype(np.float32), np.tile(up[:, slots].T, (1, NC)).astype(np.float32)


DOWN, UP = factors()
MOMENTS = [float(m) for m in np.float32(0.05) * np.exp(np.float32(0.3) * np.arange(NT, dtype=np.float32))]


def moved(x, axes):
    return lax.all_to_all(x, axes, split_axis=0, concat_axis=0, tiled=True)


def power_of(x):
    top = jnp.max(jnp.abs(x), axis=-1, keepdims=True)
    return jnp.ceil(jnp.log2(jnp.maximum(top, 1e-30))) - 14.0


def lanes(x):
    return lax.broadcasted_iota(jnp.int32, x.shape, x.ndim - 1)


def spread(x):
    power = power_of(x)
    scaled = x * jnp.exp2(-power)
    wide = scaled * 8193.0
    high = wide - (wide - scaled)
    lane = lanes(x)
    scaled = jnp.where(lane < 64, high, jnp.where(lane < 128, scaled - high, scaled))
    return jnp.where(lane == SPARE, power, scaled)


def unpacked(y):
    power = y[:, SPARE : SPARE + 1]
    return jnp.where(lanes(y) == SPARE, 0.0, y) * jnp.exp2(power)


def two_parts(x):
    high = x.astype(bf16)
    return high, (x - high.astype(f32)).astype(bf16)


def product_of(x, y):
    (a, b), (c, d) = x, y
    total = jnp.dot(a, c, preferred_element_type=f32)
    total += jnp.dot(a, d, preferred_element_type=f32)
    return total + jnp.dot(b, c, preferred_element_type=f32)


def pick_body(cols_ref, occ_ref, vir_ref, out_ref):
    points, no = occ_ref.shape
    base = lax.axis_index(YZ) * points
    slot = lax.broadcasted_iota(jnp.int32, (SLOTS, points), 0)
    place = lax.broadcasted_iota(jnp.int32, (SLOTS, points), 1)
    where = jnp.full((SLOTS, points), -1, jnp.int32)
    found = jnp.int32(0)
    for c in range(NC):
        row = cols_ref[c] - base
        here = (row >= 0) & (row < points)
        where = jnp.where(slot == jnp.where(here, found, -1), row, where)
        found = found + here.astype(jnp.int32)
    chosen = (where == place).astype(f32).astype(bf16)
    occ = jnp.dot(chosen, occ_ref[...], preferred_element_type=f32).astype(bf16)
    vir = jnp.dot(chosen, vir_ref[...], preferred_element_type=f32).astype(bf16)
    for k in range(out_ref.shape[0]):
        out_ref[k, :, :no] = occ
        out_ref[k, :, no:] = vir


def on_chip(body, shape, dtype, *args, scratch=(), last=False, count=0):
    space = pl.BlockSpec(memory_space=pltpu.VMEM)
    out = jax.ShapeDtypeStruct(shape, dtype) if last else pltpu.VMEM(shape, dtype)
    return pl.pallas_call(
        body,
        out_shape=(out,) * count if count else out,
        in_specs=[space] * len(args),
        out_specs=(space,) * count if count else space,
        scratch_shapes=scratch,
        compiler_params=pltpu.CompilerParams(vmem_limit_bytes=VMEM_LIMIT),
    )(*[pltpu.with_memory_space_constraint(jnp.asarray(a), pltpu.VMEM) for a in args])


def green_part(panel, energy, orbitals, scaled_ref, no):
    for t in range(NT):
        scaled_ref[t * NC : (t + 1) * NC, :] = (panel * jnp.exp(-energy * MOMENTS[t])).astype(bf16)
    flipped = (((1,), (1,)), ((), ()))
    occ = lax.dot_general(orbitals[:, :no], scaled_ref[:, :no], flipped, preferred_element_type=f32)
    return occ, lax.dot_general(orbitals[:, no:], scaled_ref[:, no:], flipped, preferred_element_type=f32)


def energy_of(rows):
    return sum(rows[k : k + 1].astype(f32) for k in range(3))


def offer_body(occ_ref, vir_ref, energy_ref, *out_refs):
    me = lax.axis_index(QUARTET)
    no = occ_ref.shape[1]
    quarter = out_refs[0].shape[0] - 8
    for k, out_ref in enumerate(out_refs):
        rows = pl.ds(pl.multiple_of((me ^ k) * quarter, quarter), quarter)
        out_ref[:quarter, :no] = occ_ref[rows, :]
        out_ref[:quarter, no:] = vir_ref[rows, :]
        out_ref[quarter:, :] = energy_ref[...]


def green_body(no, panels_ref, *refs):
    *theirs_refs, out_ref, scaled_ref = refs
    me = lax.axis_index(QUARTET)
    times = NT * NC
    quarter = out_ref.shape[0]
    occ, vir = 0.0, 0.0
    for k, theirs_ref in enumerate(theirs_refs):
        panel = panels_ref[me ^ k].astype(f32)
        energy = energy_of(theirs_ref[quarter:, :])
        one, two = green_part(panel, energy, theirs_ref[:quarter, :], scaled_ref.at[k], no)
        occ, vir = occ + one, vir + two
    power = jnp.maximum(power_of(occ), power_of(vir))
    factor = jnp.exp2(-power)
    out_ref[:, :times] = occ * factor
    out_ref[:, times : 2 * times] = vir * factor
    out_ref[:, 2 * times :] = jnp.broadcast_to(power, (occ.shape[0], 128))


def polar_body(got_ref, down_ref, out_ref, table_ref):
    times = NT * NC
    occ, vir = 0.0, 0.0
    for k in range(got_ref.shape[0]):
        factor = jnp.exp2(got_ref[k, :, 2 * times : 2 * times + 1])
        occ += got_ref[k, :, :times] * factor
        vir += got_ref[k, :, times : 2 * times] * factor
    column = lax.broadcasted_iota(jnp.int32, (NC, WIDTH), 0)
    same = (column == lax.broadcasted_iota(jnp.int32, (NC, WIDTH), 1) % NC).astype(f32)
    for t in range(NT):
        table_ref[t * NC : (t + 1) * NC, :] = same * down_ref[t : t + 1, :]
    out_ref[...] = spread(product_of(two_parts(occ * vir), two_parts(table_ref[...])))


def screen_body(coulomb_ref, polar_ref, out_ref):
    polar = unpacked(polar_ref[...])
    pair = polar[:, :128]
    polar = two_parts(jnp.concatenate([pair + pltpu.roll(pair, 64, 1), polar[:, 128:]], axis=1))
    step = 256
    for at in range(0, out_ref.shape[0], step):
        block = two_parts(coulomb_ref[:, at : at + step].T)
        out_ref[at : at + step, :] = spread(product_of(block, polar))


def total_body(blocks_ref, up_ref, out_ref, table_ref):
    total = 0.0
    for k in range(blocks_ref.shape[0]):
        total += unpacked(blocks_ref[k])
    column = lax.broadcasted_iota(jnp.int32, (NC, NC * NF), 0)
    same = (column == lax.broadcasted_iota(jnp.int32, (NC, NC * NF), 1) // NF).astype(f32)
    for k in range(WIDTH // NC):
        table_ref[k * NC : (k + 1) * NC, :] = same * up_ref[k : k + 1, :]
    out_ref[...] = product_of(two_parts(total), two_parts(table_ref[...]))


def panel_rows(panel_cols, occ_orbitals, vir_orbitals):
    points, no = occ_orbitals.shape
    width = no + vir_orbitals.shape[1]
    blocks = lax.axis_size(YZ)
    sent = pl.pallas_call(
        pick_body,
        out_shape=jax.ShapeDtypeStruct((blocks, SLOTS, width), bf16),
        in_specs=[pl.BlockSpec(memory_space=pltpu.SMEM)] + [pl.BlockSpec(memory_space=pltpu.VMEM)] * 2,
        compiler_params=pltpu.CompilerParams(vmem_limit_bytes=VMEM_LIMIT),
    )(panel_cols, occ_orbitals, vir_orbitals)
    got = moved(sent, YZ).reshape(blocks * SLOTS, width)
    block = panel_cols // points
    earlier = np.tril(np.ones((NC, NC), bool), -1)
    slot = ((block[:, None] == block[None, :]) & earlier).astype(jnp.int32).sum(axis=1)
    source = lax.broadcasted_iota(jnp.int32, (NC, blocks * SLOTS), 1)
    chosen = ((block * SLOTS + slot)[:, None] == source).astype(bf16)
    few = jnp.dot(chosen, got, preferred_element_type=f32)

    def summed():
        zs = lax.axis_size("z")
        positions = lax.broadcasted_iota(jnp.int32, (NC, points), 1)
        selector = (panel_cols[:, None] - lax.axis_index(YZ) * points == positions).astype(bf16)
        pick = [jnp.dot(selector, o, preferred_element_type=f32).astype(bf16) for o in (occ_orbitals, vir_orbitals)]
        pick = jnp.concatenate(pick, axis=1).reshape(zs, NC // zs, width)
        own = moved(pick, "z").astype(f32).sum(axis=0).astype(bf16)
        rows = moved(jnp.broadcast_to(own, (blocks, *own.shape)), YZ)
        return rows.reshape(-1, NC, width).astype(f32).sum(axis=0)

    return lax.cond(jnp.any(slot >= SLOTS), summed, lambda: few), sent


def in_three(e):
    hi = lax.reduce_precision(e, 8, 7)
    mid = lax.reduce_precision(e - hi, 8, 7)
    return jnp.stack([hi, mid, e - hi - mid]).astype(bf16)


def local(panel_cols, occ_orbitals, vir_orbitals, occ_energy, vir_energy, coulomb):
    points, no = occ_orbitals.shape
    members = lax.axis_size(QUARTET)
    quarter = points // members
    times = NT * NC

    panel, picked = panel_rows(panel_cols, occ_orbitals, vir_orbitals)
    width = panel.shape[1]
    occ_late, vir_late, _ = lax.optimization_barrier((occ_orbitals, vir_orbitals, picked))
    energies = jnp.pad(in_three(jnp.concatenate([occ_energy, vir_energy])), ((0, 5), (0, 0)))
    mine, *others = on_chip(offer_body, (quarter + 8, width), bf16, occ_late, vir_late, energies, count=members)
    theirs = [
        lax.ppermute(x, QUARTET, [(i, i ^ k) for i in range(members)]) for k, x in enumerate(others, start=1)
    ]
    panel, *theirs = lax.optimization_barrier((panel, *theirs))
    panels = moved(jnp.broadcast_to(panel.astype(bf16), (members, *panel.shape)), QUARTET)
    sent = on_chip(
        functools.partial(green_body, no),
        (quarter, 2 * times + 128),
        f32,
        panels,
        mine,
        *theirs,
        scratch=[pltpu.VMEM((members, times, width), bf16)],
    ).astype(f16)
    got = moved(sent.reshape(lax.axis_size("x"), -1, 2 * times + 128), "x")
    table = [pltpu.VMEM((times, WIDTH), f32)]
    polar = on_chip(polar_body, (got.shape[1], WIDTH), f32, got.astype(f32), DOWN, scratch=table).astype(f16)
    polar = moved(jnp.broadcast_to(polar, (lax.axis_size(ORB), *polar.shape)), (*QUARTET, "x"))
    polar = polar.reshape(points, WIDTH).astype(f32)
    part = on_chip(screen_body, (coulomb.shape[1], WIDTH), f32, coulomb, polar).astype(f16)
    blocks = moved(part.reshape(NC, -1, WIDTH), YZ).astype(f32)
    table = [pltpu.VMEM((WIDTH, NC * NF), f32)]
    return on_chip(total_body, (blocks.shape[1], NC * NF), f32, blocks, UP, scratch=table, last=True)


def solution(mesh):
    finer = Mesh(mesh.devices.reshape(4, 8, 4, 2, 2), (*YZ, *ORB))
    placed = (P(), P(YZ, ORB), P(YZ, ORB), P(ORB), P(ORB), P(YZ, ORB))
    return jax.shard_map(local, mesh=finer, in_specs=placed, out_specs=P(ORB + YZ, None), check_vma=False)
```

```python
import jax
import jax.numpy as jnp
import numpy as np
from jax import lax
from jax.experimental import pallas as pl
from jax.experimental.pallas import tpu as pltpu
from jax.sharding import Mesh
from jax.sharding import PartitionSpec as P

NT = 16
NF = 16
NC = 32
RANK = 10
TWICE = 2
WIDTH = 384
SPARE = 127
SLOTS = 8
VMEM_LIMIT = 12 * 2**20
YZ = ("yh", "z")
ORB = ("x", "yl", "core")
f32, f16, bf16 = jnp.float32, jnp.float16, jnp.bfloat16


def factors():
    moments = 0.05 * np.exp(0.3 * np.arange(NT))
    freqs = 0.1 * np.exp(0.3 * np.arange(NF))
    table = 0.3 * moments[None, :] * np.cos(freqs[:, None] * moments[None, :])
    u = np.linalg.svd(table)[0][:, :RANK]
    rates = np.exp(np.linspace(np.log(0.1), np.log(5.0), 400))
    typical = u.T @ table @ np.exp(-moments[:, None] * rates[None, :])
    turn = np.linalg.eigh(typical @ typical.T)[1][:, ::-1]
    up = u @ turn
    down = up.T @ table
    slots = [*range(TWICE), *range(TWICE), *range(TWICE, RANK)]
    return np.repeat(down[slots].T, NC, axis=1).astype(np.float32), np.tile(up[:, slots].T, (1, NC)).astype(np.float32)


DOWN, UP = factors()
MOMENTS = [float(m) for m in np.float32(0.05) * np.exp(np.float32(0.3) * np.arange(NT, dtype=np.float32))]


def moved(x, axes):
    return lax.all_to_all(x, axes, split_axis=0, concat_axis=0, tiled=True)


def power_of(x):
    top = jnp.max(jnp.abs(x), axis=-1, keepdims=True)
    return jnp.ceil(jnp.log2(jnp.maximum(top, 1e-30))) - 14.0


def lanes(x):
    return lax.broadcasted_iota(jnp.int32, x.shape, x.ndim - 1)


def spread(x):
    power = power_of(x)
    scaled = x * jnp.exp2(-power)
    wide = scaled * 8193.0
    high = wide - (wide - scaled)
    lane = lanes(x)
    scaled = jnp.where(lane < 64, high, jnp.where(lane < 128, scaled - high, scaled))
    return jnp.where(lane == SPARE, power, scaled)


def unpacked(y):
    power = y[:, SPARE : SPARE + 1]
    return jnp.where(lanes(y) == SPARE, 0.0, y) * jnp.exp2(power)


def two_parts(x):
    high = x.astype(bf16)
    return high, (x - high.astype(f32)).astype(bf16)


def product_of(x, y):
    (a, b), (c, d) = x, y
    total = jnp.dot(a, c, preferred_element_type=f32)
    total += jnp.dot(a, d, preferred_element_type=f32)
    return total + jnp.dot(b, c, preferred_element_type=f32)


def pick_body(cols_ref, occ_ref, vir_ref, out_ref):
    points, no = occ_ref.shape
    base = lax.axis_index(YZ) * points
    slot = lax.broadcasted_iota(jnp.int32, (SLOTS, points), 0)
    place = lax.broadcasted_iota(jnp.int32, (SLOTS, points), 1)
    where = jnp.full((SLOTS, points), -1, jnp.int32)
    found = jnp.int32(0)
    for c in range(NC):
        row = cols_ref[c] - base
        here = (row >= 0) & (row < points)
        where = jnp.where(slot == jnp.where(here, found, -1), row, where)
        found = found + here.astype(jnp.int32)
    chosen = (where == place).astype(f32).astype(bf16)
    occ = jnp.dot(chosen, occ_ref[...], preferred_element_type=f32).astype(bf16)
    vir = jnp.dot(chosen, vir_ref[...], preferred_element_type=f32).astype(bf16)
    for k in range(out_ref.shape[0]):
        out_ref[k, :, :no] = occ
        out_ref[k, :, no:] = vir


def on_chip(body, shape, dtype, *args, scratch=(), last=False):
    space = pl.BlockSpec(memory_space=pltpu.VMEM)
    return pl.pallas_call(
        body,
        out_shape=jax.ShapeDtypeStruct(shape, dtype) if last else pltpu.VMEM(shape, dtype),
        in_specs=[space] * len(args),
        out_specs=space,
        scratch_shapes=scratch,
        compiler_params=pltpu.CompilerParams(vmem_limit_bytes=VMEM_LIMIT),
    )(*[pltpu.with_memory_space_constraint(jnp.asarray(a), pltpu.VMEM) for a in args])


def green_part(panel, occ_energy, vir_energy, occ, vir, scaled_ref):
    no = occ.shape[1]
    for energy, at in ((occ_energy, slice(0, no)), (vir_energy, slice(no, None))):
        for t in range(NT):
            decay = jnp.exp(-energy * MOMENTS[t])
            scaled_ref[t * NC : (t + 1) * NC, at] = (panel[:, at] * decay).astype(bf16)
    flipped = (((1,), (1,)), ((), ()))
    return (
        lax.dot_general(occ, scaled_ref[:, :no], flipped, preferred_element_type=f32),
        lax.dot_general(vir, scaled_ref[:, no:], flipped, preferred_element_type=f32),
    )


def green_body(panel_ref, other_panel_ref, occ_e_ref, vir_e_ref, other_e_ref, occ_ref, vir_ref, theirs_ref, out_ref, scaled_ref):
    times, no = NT * NC, occ_ref.shape[1]
    half = occ_ref.shape[0]
    occ, vir = green_part(panel_ref[...], occ_e_ref[...], vir_e_ref[...], occ_ref[...], vir_ref[...], scaled_ref.at[0])
    energy, theirs = other_e_ref[...], theirs_ref[:half]
    other_occ, other_vir = green_part(
        other_panel_ref[...].astype(f32),
        energy[:, :no],
        energy[:, no:],
        theirs[:, :no],
        theirs[:, no:],
        scaled_ref.at[1],
    )
    occ, vir = occ + other_occ, vir + other_vir
    power = jnp.maximum(power_of(occ), power_of(vir))
    factor = jnp.exp2(-power)
    out_ref[:, :times] = occ * factor
    out_ref[:, times : 2 * times] = vir * factor
    out_ref[:, 2 * times :] = jnp.broadcast_to(power, (occ.shape[0], 128))


def polar_body(got_ref, down_ref, out_ref, table_ref):
    times = NT * NC
    occ, vir = 0.0, 0.0
    for k in range(got_ref.shape[0]):
        factor = jnp.exp2(got_ref[k, :, 2 * times : 2 * times + 1])
        occ += got_ref[k, :, :times] * factor
        vir += got_ref[k, :, times : 2 * times] * factor
    column = lax.broadcasted_iota(jnp.int32, (NC, WIDTH), 0)
    same = (column == lax.broadcasted_iota(jnp.int32, (NC, WIDTH), 1) % NC).astype(f32)
    for t in range(NT):
        table_ref[t * NC : (t + 1) * NC, :] = same * down_ref[t : t + 1, :]
    out_ref[...] = spread(product_of(two_parts(occ * vir), two_parts(table_ref[...])))


def screen_body(coulomb_ref, polar_ref, out_ref):
    polar = unpacked(polar_ref[...])
    pair = polar[:, :128]
    polar = two_parts(jnp.concatenate([pair + pltpu.roll(pair, 64, 1), polar[:, 128:]], axis=1))
    step = 256
    for at in range(0, out_ref.shape[0], step):
        block = two_parts(coulomb_ref[:, at : at + step].T)
        out_ref[at : at + step, :] = spread(product_of(block, polar))


def total_body(blocks_ref, up_ref, out_ref, table_ref):
    total = 0.0
    for k in range(blocks_ref.shape[0]):
        total += unpacked(blocks_ref[k])
    column = lax.broadcasted_iota(jnp.int32, (NC, NC * NF), 0)
    same = (column == lax.broadcasted_iota(jnp.int32, (NC, NC * NF), 1) // NF).astype(f32)
    for k in range(WIDTH // NC):
        table_ref[k * NC : (k + 1) * NC, :] = same * up_ref[k : k + 1, :]
    out_ref[...] = product_of(two_parts(total), two_parts(table_ref[...]))


def panel_rows(panel_cols, occ_orbitals, vir_orbitals):
    points, no = occ_orbitals.shape
    width = no + vir_orbitals.shape[1]
    blocks = lax.axis_size(YZ)
    sent = pl.pallas_call(
        pick_body,
        out_shape=jax.ShapeDtypeStruct((blocks, SLOTS, width), bf16),
        in_specs=[pl.BlockSpec(memory_space=pltpu.SMEM)] + [pl.BlockSpec(memory_space=pltpu.VMEM)] * 2,
        compiler_params=pltpu.CompilerParams(vmem_limit_bytes=VMEM_LIMIT),
    )(panel_cols, occ_orbitals, vir_orbitals)
    got = moved(sent, YZ).reshape(blocks * SLOTS, width)
    block = panel_cols // points
    earlier = np.tril(np.ones((NC, NC), bool), -1)
    slot = ((block[:, None] == block[None, :]) & earlier).astype(jnp.int32).sum(axis=1)
    source = lax.broadcasted_iota(jnp.int32, (NC, blocks * SLOTS), 1)
    chosen = ((block * SLOTS + slot)[:, None] == source).astype(bf16)
    few = jnp.dot(chosen, got, preferred_element_type=f32)

    def summed():
        zs = lax.axis_size("z")
        positions = lax.broadcasted_iota(jnp.int32, (NC, points), 1)
        selector = (panel_cols[:, None] - lax.axis_index(YZ) * points == positions).astype(bf16)
        pick = [jnp.dot(selector, o, preferred_element_type=f32).astype(bf16) for o in (occ_orbitals, vir_orbitals)]
        pick = jnp.concatenate(pick, axis=1).reshape(zs, NC // zs, width)
        own = moved(pick, "z").astype(f32).sum(axis=0).astype(bf16)
        rows = moved(jnp.broadcast_to(own, (blocks, *own.shape)), YZ)
        return rows.reshape(-1, NC, width).astype(f32).sum(axis=0)

    return lax.cond(jnp.any(slot >= SLOTS), summed, lambda: few), sent


def in_three(e):
    hi = lax.reduce_precision(e, 8, 7)
    mid = lax.reduce_precision(e - hi, 8, 7)
    return jnp.stack([hi, mid, e - hi - mid]).astype(bf16)


def to_other_core(x):
    return lax.ppermute(x, "core", [(0, 1), (1, 0)])


def local(panel_cols, occ_orbitals, vir_orbitals, occ_energy, vir_energy, coulomb):
    points, no = occ_orbitals.shape
    half = points // 2
    times = NT * NC
    core = lax.axis_index("core")

    def rows_of(x, k):
        return jnp.where(k == 0, x[:half], x[half:])

    panel, picked = panel_rows(panel_cols, occ_orbitals, vir_orbitals)
    occ_late, vir_late, _ = lax.optimization_barrier((occ_orbitals, vir_orbitals, picked))
    energies = in_three(jnp.concatenate([occ_energy, vir_energy]))
    theirs = jnp.concatenate([rows_of(occ_late, 1 - core), rows_of(vir_late, 1 - core)], axis=1)
    theirs = jnp.concatenate([theirs, jnp.pad(energies, ((0, 5), (0, 0)))], axis=0)
    theirs = to_other_core(theirs)
    pieces = theirs[half : half + 3].astype(f32)
    other_energy = pieces[0:1] + pieces[1:2] + pieces[2:3]
    other_panel = to_other_core(panel.astype(bf16))
    sent = on_chip(
        green_body,
        (half, 2 * times + 128),
        f32,
        panel,
        other_panel,
        occ_energy.reshape(1, -1),
        vir_energy.reshape(1, -1),
        other_energy,
        rows_of(occ_late, core),
        rows_of(vir_late, core),
        theirs,
        scratch=[pltpu.VMEM((2, times, panel.shape[1]), bf16)],
    ).astype(f16)
    peers = lax.axis_size(("x", "yl"))
    got = moved(sent.reshape(peers, half // peers, -1), ("x", "yl"))
    table = [pltpu.VMEM((times, WIDTH), f32)]
    polar = on_chip(polar_body, (got.shape[1], WIDTH), f32, got.astype(f32), DOWN, scratch=table).astype(f16)
    polar = moved(jnp.broadcast_to(polar, (lax.axis_size(ORB), *polar.shape)), ("core", "x", "yl"))
    polar = polar.reshape(points, WIDTH).astype(f32)
    part = on_chip(screen_body, (coulomb.shape[1], WIDTH), f32, coulomb, polar).astype(f16)
    blocks = moved(part.reshape(NC, -1, WIDTH), YZ).astype(f32)
    table = [pltpu.VMEM((WIDTH, NC * NF), f32)]
    return on_chip(total_body, (blocks.shape[1], NC * NF), f32, blocks, UP, scratch=table, last=True)


def solution(mesh):
    finer = Mesh(mesh.devices.reshape(4, 8, 4, 2, 2), (*YZ, *ORB))
    placed = (P(), P(YZ, ORB), P(YZ, ORB), P(ORB), P(ORB), P(YZ, ORB))
    return jax.shard_map(local, mesh=finer, in_specs=placed, out_specs=P(ORB + YZ, None), check_vma=False)
```

```python
import functools

import jax
import jax.numpy as jnp
import numpy as np
from jax import lax
from jax.experimental import pallas as pl
from jax.experimental.pallas import tpu as pltpu
from jax.sharding import Mesh
from jax.sharding import PartitionSpec as P

NT = 16
NF = 16
NC = 32
RANK = 10
TWICE = 2
WIDTH = 384
SPARE = 127
SLOTS = 8
VMEM_LIMIT = 12 * 2**20
YZ = ("yh", "z")
ORB = ("x", "yl", "core")
QUARTET = ("yl", "core")
f32, f16, bf16 = jnp.float32, jnp.float16, jnp.bfloat16


def factors():
    moments = 0.05 * np.exp(0.3 * np.arange(NT))
    freqs = 0.1 * np.exp(0.3 * np.arange(NF))
    table = 0.3 * moments[None, :] * np.cos(freqs[:, None] * moments[None, :])
    u = np.linalg.svd(table)[0][:, :RANK]
    rates = np.exp(np.linspace(np.log(0.1), np.log(5.0), 400))
    typical = u.T @ table @ np.exp(-moments[:, None] * rates[None, :])
    turn = np.linalg.eigh(typical @ typical.T)[1][:, ::-1]
    up = u @ turn
    down = up.T @ table
    slots = [*range(TWICE), *range(TWICE), *range(TWICE, RANK)]
    return np.repeat(down[slots].T, NC, axis=1).astype(np.float32), np.tile(up[:, slots].T, (1, NC)).astype(np.float32)


DOWN, UP = factors()
MOMENTS = [float(m) for m in np.float32(0.05) * np.exp(np.float32(0.3) * np.arange(NT, dtype=np.float32))]


def moved(x, axes):
    return lax.all_to_all(x, axes, split_axis=0, concat_axis=0, tiled=True)


def power_of(x):
    top = jnp.max(jnp.abs(x), axis=-1, keepdims=True)
    return jnp.ceil(jnp.log2(jnp.maximum(top, 1e-30))) - 14.0


def lanes(x):
    return lax.broadcasted_iota(jnp.int32, x.shape, x.ndim - 1)


def spread(x):
    power = power_of(x)
    scaled = x * jnp.exp2(-power)
    wide = scaled * 8193.0
    high = wide - (wide - scaled)
    lane = lanes(x)
    scaled = jnp.where(lane < 64, high, jnp.where(lane < 128, scaled - high, scaled))
    return jnp.where(lane == SPARE, power, scaled)


def unpacked(y):
    power = y[:, SPARE : SPARE + 1]
    return jnp.where(lanes(y) == SPARE, 0.0, y) * jnp.exp2(power)


def two_parts(x):
    high = x.astype(bf16)
    return high, (x - high.astype(f32)).astype(bf16)


def product_of(x, y):
    (a, b), (c, d) = x, y
    total = jnp.dot(a, c, preferred_element_type=f32)
    total += jnp.dot(a, d, preferred_element_type=f32)
    return total + jnp.dot(b, c, preferred_element_type=f32)


def pick_body(cols_ref, occ_ref, vir_ref, out_ref):
    points, no = occ_ref.shape
    base = lax.axis_index(YZ) * points
    slot = lax.broadcasted_iota(jnp.int32, (SLOTS, points), 0)
    place = lax.broadcasted_iota(jnp.int32, (SLOTS, points), 1)
    where = jnp.full((SLOTS, points), -1, jnp.int32)
    found = jnp.int32(0)
    for c in range(NC):
        row = cols_ref[c] - base
        here = (row >= 0) & (row < points)
        where = jnp.where(slot == jnp.where(here, found, -1), row, where)
        found = found + here.astype(jnp.int32)
    chosen = (where == place).astype(f32).astype(bf16)
    occ = jnp.dot(chosen, occ_ref[...], preferred_element_type=f32).astype(bf16)
    vir = jnp.dot(chosen, vir_ref[...], preferred_element_type=f32).astype(bf16)
    for k in range(out_ref.shape[0]):
        out_ref[k, :, :no] = occ
        out_ref[k, :, no:] = vir


def on_chip(body, shape, dtype, *args, scratch=(), last=False, count=0):
    space = pl.BlockSpec(memory_space=pltpu.VMEM)
    out = jax.ShapeDtypeStruct(shape, dtype) if last else pltpu.VMEM(shape, dtype)
    return pl.pallas_call(
        body,
        out_shape=(out,) * count if count else out,
        in_specs=[space] * len(args),
        out_specs=(space,) * count if count else space,
        scratch_shapes=scratch,
        compiler_params=pltpu.CompilerParams(vmem_limit_bytes=VMEM_LIMIT),
    )(*[pltpu.with_memory_space_constraint(jnp.asarray(a), pltpu.VMEM) for a in args])


def green_part(panel, energy, orbitals, scaled_ref, no):
    for t in range(NT):
        scaled_ref[t * NC : (t + 1) * NC, :] = (panel * jnp.exp(-energy * MOMENTS[t])).astype(bf16)
    flipped = (((1,), (1,)), ((), ()))
    occ = lax.dot_general(orbitals[:, :no], scaled_ref[:, :no], flipped, preferred_element_type=f32)
    return occ, lax.dot_general(orbitals[:, no:], scaled_ref[:, no:], flipped, preferred_element_type=f32)


def energy_of(rows):
    return sum(rows[k : k + 1].astype(f32) for k in range(3))


def offer_body(occ_ref, vir_ref, energy_ref, *out_refs):
    me = lax.axis_index(QUARTET)
    points, no = occ_ref.shape
    quarter = points // len(out_refs)
    run = quarter // lax.axis_size("x")
    for k, out_ref in enumerate(out_refs):
        for x in range(quarter // run):
            rows = pl.ds(pl.multiple_of(x * quarter + (me ^ k) * run, run), run)
            out_ref[x * run : (x + 1) * run, :no] = occ_ref[rows, :]
            out_ref[x * run : (x + 1) * run, no:] = vir_ref[rows, :]
        out_ref[quarter:, :] = energy_ref[...]


def green_body(no, panels_ref, *refs):
    *theirs_refs, out_ref, scaled_ref = refs
    me = lax.axis_index(QUARTET)
    times = NT * NC
    quarter = out_ref.shape[0]
    occ, vir = 0.0, 0.0
    for k, theirs_ref in enumerate(theirs_refs):
        panel = panels_ref[me ^ k].astype(f32)
        energy = energy_of(theirs_ref[quarter:, :])
        one, two = green_part(panel, energy, theirs_ref[:quarter, :], scaled_ref.at[k], no)
        occ, vir = occ + one, vir + two
    power = jnp.maximum(power_of(occ), power_of(vir))
    factor = jnp.exp2(-power)
    out_ref[:, :times] = occ * factor
    out_ref[:, times : 2 * times] = vir * factor
    out_ref[:, 2 * times :] = jnp.broadcast_to(power, (occ.shape[0], 128))


def polar_body(got_ref, down_ref, out_ref, table_ref):
    times = NT * NC
    occ, vir = 0.0, 0.0
    for k in range(got_ref.shape[0]):
        factor = jnp.exp2(got_ref[k, :, 2 * times : 2 * times + 1])
        occ += got_ref[k, :, :times] * factor
        vir += got_ref[k, :, times : 2 * times] * factor
    column = lax.broadcasted_iota(jnp.int32, (NC, WIDTH), 0)
    same = (column == lax.broadcasted_iota(jnp.int32, (NC, WIDTH), 1) % NC).astype(f32)
    for t in range(NT):
        table_ref[t * NC : (t + 1) * NC, :] = same * down_ref[t : t + 1, :]
    out_ref[...] = spread(product_of(two_parts(occ * vir), two_parts(table_ref[...])))


def screen_body(coulomb_ref, polar_ref, out_ref):
    polar = unpacked(polar_ref[...])
    pair = polar[:, :128]
    polar = two_parts(jnp.concatenate([pair + pltpu.roll(pair, 64, 1), polar[:, 128:]], axis=1))
    step = 256
    for at in range(0, out_ref.shape[0], step):
        block = two_parts(coulomb_ref[:, at : at + step].T)
        out_ref[at : at + step, :] = spread(product_of(block, polar))


def total_body(blocks_ref, up_ref, out_ref, table_ref):
    total = 0.0
    for k in range(blocks_ref.shape[0]):
        total += unpacked(blocks_ref[k])
    column = lax.broadcasted_iota(jnp.int32, (NC, NC * NF), 0)
    same = (column == lax.broadcasted_iota(jnp.int32, (NC, NC * NF), 1) // NF).astype(f32)
    for k in range(WIDTH // NC):
        table_ref[k * NC : (k + 1) * NC, :] = same * up_ref[k : k + 1, :]
    out_ref[...] = product_of(two_parts(total), two_parts(table_ref[...]))


def panel_rows(panel_cols, occ_orbitals, vir_orbitals):
    points, no = occ_orbitals.shape
    width = no + vir_orbitals.shape[1]
    blocks = lax.axis_size(YZ)
    sent = pl.pallas_call(
        pick_body,
        out_shape=jax.ShapeDtypeStruct((blocks, SLOTS, width), bf16),
        in_specs=[pl.BlockSpec(memory_space=pltpu.SMEM)] + [pl.BlockSpec(memory_space=pltpu.VMEM)] * 2,
        compiler_params=pltpu.CompilerParams(vmem_limit_bytes=VMEM_LIMIT),
    )(panel_cols, occ_orbitals, vir_orbitals)
    got = moved(sent, YZ).reshape(blocks * SLOTS, width)
    block = panel_cols // points
    earlier = np.tril(np.ones((NC, NC), bool), -1)
    slot = ((block[:, None] == block[None, :]) & earlier).astype(jnp.int32).sum(axis=1)
    source = lax.broadcasted_iota(jnp.int32, (NC, blocks * SLOTS), 1)
    chosen = ((block * SLOTS + slot)[:, None] == source).astype(bf16)
    few = jnp.dot(chosen, got, preferred_element_type=f32)

    def summed():
        zs = lax.axis_size("z")
        positions = lax.broadcasted_iota(jnp.int32, (NC, points), 1)
        selector = (panel_cols[:, None] - lax.axis_index(YZ) * points == positions).astype(bf16)
        pick = [jnp.dot(selector, o, preferred_element_type=f32).astype(bf16) for o in (occ_orbitals, vir_orbitals)]
        pick = jnp.concatenate(pick, axis=1).reshape(zs, NC // zs, width)
        own = moved(pick, "z").astype(f32).sum(axis=0).astype(bf16)
        rows = moved(jnp.broadcast_to(own, (blocks, *own.shape)), YZ)
        return rows.reshape(-1, NC, width).astype(f32).sum(axis=0)

    return lax.cond(jnp.any(slot >= SLOTS), summed, lambda: few), sent


def in_three(e):
    hi = lax.reduce_precision(e, 8, 7)
    mid = lax.reduce_precision(e - hi, 8, 7)
    return jnp.stack([hi, mid, e - hi - mid]).astype(bf16)


def local(panel_cols, occ_orbitals, vir_orbitals, occ_energy, vir_energy, coulomb):
    points, no = occ_orbitals.shape
    members = lax.axis_size(QUARTET)
    quarter = points // members
    times = NT * NC

    panel, picked = panel_rows(panel_cols, occ_orbitals, vir_orbitals)
    width = panel.shape[1]
    occ_late, vir_late, _ = lax.optimization_barrier((occ_orbitals, vir_orbitals, picked))
    energies = jnp.pad(in_three(jnp.concatenate([occ_energy, vir_energy])), ((0, 5), (0, 0)))
    mine, *others = on_chip(offer_body, (quarter + 8, width), bf16, occ_late, vir_late, energies, count=members)
    theirs = [
        lax.ppermute(x, QUARTET, [(i, i ^ k) for i in range(members)]) for k, x in enumerate(others, start=1)
    ]
    panel, *theirs = lax.optimization_barrier((panel, *theirs))
    panels = moved(jnp.broadcast_to(panel.astype(bf16), (members, *panel.shape)), QUARTET)
    sent = on_chip(
        functools.partial(green_body, no),
        (quarter, 2 * times + 128),
        f32,
        panels,
        mine,
        *theirs,
        scratch=[pltpu.VMEM((members, times, width), bf16)],
    ).astype(f16)
    got = moved(sent.reshape(lax.axis_size("x"), -1, 2 * times + 128), "x")
    table = [pltpu.VMEM((times, WIDTH), f32)]
    polar = on_chip(polar_body, (got.shape[1], WIDTH), f32, got.astype(f32), DOWN, scratch=table).astype(f16)
    polar = moved(jnp.broadcast_to(polar, (lax.axis_size(ORB), *polar.shape)), ORB)
    polar = polar.reshape(points, WIDTH).astype(f32)
    part = on_chip(screen_body, (coulomb.shape[1], WIDTH), f32, coulomb, polar).astype(f16)
    blocks = moved(part.reshape(NC, -1, WIDTH), YZ).astype(f32)
    table = [pltpu.VMEM((WIDTH, NC * NF), f32)]
    return on_chip(total_body, (blocks.shape[1], NC * NF), f32, blocks, UP, scratch=table, last=True)


def solution(mesh):
    finer = Mesh(mesh.devices.reshape(4, 8, 4, 2, 2), (*YZ, *ORB))
    placed = (P(), P(YZ, ORB), P(YZ, ORB), P(ORB), P(ORB), P(YZ, ORB))
    return jax.shard_map(local, mesh=finer, in_specs=placed, out_specs=P(ORB + YZ, None), check_vma=False)
```
